32 devices in a mesh: re: 4 (over y, x), ka: 8 (over z, core).
Axes of the slice: x: 2, y: 2, z: 4, core: 2. Of those that a mesh axis runs over, the one named last changes fastest.
Arguments:
- lattice_blocks: bfloat16 [192, 2, 3, 256], P(('re', 'ka')), may hold values from -0.4375 to 0.4375
- lattice_coords: int32 [192, 3], P(('re', 'ka')), may hold values from -8 to 8
- kpoint_index: int32 [192, 3], P('ka'), may hold values from 0 to 63
- polarization: float32 [3], replicated, may hold values from -4 to 4
- energy_gap: float32 [192, 32], P('ka'), may hold values from 0.5 to 2.5
- coupling: bfloat16 [8, 96, 2, 32, 8], P('ka', 're'), may hold values from -1 to 1
- phonon_weight: bfloat16 [8, 96], P('ka', 're'), may hold values from 0.19921875 to 5
Outputs:
- rates: float32 [192, 8], P('ka', 're')
The draws below stay inside these ranges and needn't reach their ends.
All inputs are finite; a program needn't handle non-finite values.
Results may differ from the reference program's by a relative error of at most 0.0014.
Values may be sent and summed in bfloat16 or wider, within the bound.
A program may use at most 128 MiB of HBM per device.

```python
import math
import jax
import jax.numpy as jnp
from jax import lax

NB = 32
NV = 8
NC = 8
NMODE = 96
NKG = 64
NRE = 192
K = 192
Q = 8


def plant(drawn, key, low, high):
    dims = drawn.shape
    spot = [jax.random.randint(jax.random.fold_in(key, axis), (), 0, dims[axis]) for axis in range(len(dims))]
    drawn = drawn.at[tuple(spot)].set(low)
    longest = dims.index(max(dims))
    spot[longest] = (spot[longest] + 1) % dims[longest]
    return drawn.at[tuple(spot)].set(high)


def level_of(key, extent, shards, least, top_value):
    factor_of = 1.0
    for dim, blocks in shards:
        steps = jax.random.uniform(jax.random.fold_in(jax.random.fold_in(key, 6), dim), (blocks,), jnp.float32, least / len(shards), top_value / len(shards))
        factor_of = factor_of * jnp.repeat(jnp.exp(steps), extent[dim] // blocks).reshape((-1,) + (1,) * (len(extent) - 1 - dim))
    return factor_of


def bell_draw(rng, extent, scale, most, pieces=(), held_as=jnp.bfloat16):
    entries = scale * jax.random.normal(rng, extent, jnp.float32)
    if pieces:
        entries = entries * level_of(rng, extent, pieces, -0.22, 0.18)
    return jnp.clip(entries, -most, most).astype(held_as)


def setup_inputs(seed: int = 0) -> dict:
    key_list = jax.random.split(jax.random.key(seed), 8)
    lattice_blocks = bell_draw(key_list[0], (NRE, 2, 3, NV * NB), NRE ** -0.5, 0.4375, ((0, 32),))
    lattice_coords = plant(jax.random.randint(key_list[1], (NRE, 3), -8, 9), jax.random.fold_in(key_list[1], 1), -8, 8).astype(jnp.int32)
    kpoint_index = plant(jax.random.randint(key_list[2], (K, 3), 0, NKG), jax.random.fold_in(key_list[2], 1), 0, NKG - 1).astype(jnp.int32)
    polarization = bell_draw(key_list[3], (3,), 1.0, 4.0, (), jnp.float32)
    energy_gap = jnp.clip(0.5 + 2.0 * jax.random.uniform(key_list[4], (K, NB), jnp.float32) ** level_of(key_list[4], (K, NB), ((0, 8),), -0.2, 0.2), 0.5, 2.5)
    coupling = bell_draw(key_list[5], (Q, NMODE, 2, NB, NC), NB ** -0.5, 1.0, ((0, 8), (1, 4)))
    phonon_weight = jnp.clip(jnp.exp(math.log(5.0) - 3.2227897 * jax.random.uniform(key_list[6], (Q, NMODE), jnp.float32) ** level_of(key_list[6], (Q, NMODE), ((0, 8), (1, 4)), -0.2, 0.2)), 0.19921875, 5.0).astype(jnp.bfloat16)
    return dict(lattice_blocks=lattice_blocks, lattice_coords=lattice_coords, kpoint_index=kpoint_index, polarization=polarization, energy_gap=energy_gap, coupling=coupling, phonon_weight=phonon_weight)


def phase_rows(kpoint_index, coords):
    turns = jnp.mod(jnp.sum(kpoint_index[:, None, :] * coords[None, :, :], axis=2), NKG)
    angle = turns.astype(jnp.float32) * (2.0 * math.pi / NKG)
    cosine = jnp.cos(angle).astype(jnp.bfloat16)
    sine = jnp.sin(angle).astype(jnp.bfloat16)
    count = kpoint_index.shape[0]
    upper = jnp.stack([cosine, -sine], axis=2).reshape(count, -1)
    lower = jnp.stack([sine, cosine], axis=2).reshape(count, -1)
    return jnp.concatenate([upper, lower], axis=0)


def left_factor(momenta, polarization, energy_gap):
    count = momenta.shape[1]
    parts = momenta.reshape(2, count, 3, NV, -1)
    along = parts[:, :, 0] * polarization[0] + parts[:, :, 1] * polarization[1] + parts[:, :, 2] * polarization[2]
    return (along / energy_gap[None, :, None, :]).astype(jnp.bfloat16).reshape(2, count * NV, -1)


def rate_block(factor, coup, weight):
    def product(left, right):
        return jnp.einsum('qvmj,am->qvja', right.astype(jnp.float32), left.astype(jnp.float32))
    real_left, imag_left = factor[0], factor[1]
    real_right, imag_right = coup[:, :, 0], coup[:, :, 1]
    are = product(real_left, real_right) - product(imag_left, imag_right)
    aim = product(real_left, imag_right) + product(imag_left, real_right)
    power = (are * are + aim * aim) * weight.astype(jnp.float32)[:, :, None, None]
    summed = jnp.sum(power, axis=(1, 2))
    count = factor.shape[1] // NV
    qcount = coup.shape[0]
    return jnp.sum(summed.reshape(qcount, count, NV), axis=2).T * (1.0 / (NMODE * NV * NC))


def reference(lattice_blocks, lattice_coords, kpoint_index, polarization, energy_gap, coupling, phonon_weight):
    count = kpoint_index.shape[0]
    left = phase_rows(kpoint_index, lattice_coords)
    cols = lattice_blocks.shape[2] * lattice_blocks.shape[3]
    momenta = jnp.dot(left, lattice_blocks.reshape(-1, cols), preferred_element_type=jnp.float32)
    factor = left_factor(momenta.reshape(2, count, cols), polarization, energy_gap)

    def per_point(pair):
        coup, weight = pair
        return rate_block(factor, coup[None], weight[None])[:, 0]

    columns = lax.map(per_point, (coupling, phonon_weight))
    return columns.T
```

```python
import functools
import math

import jax
import jax.numpy as jnp
from jax import lax
from jax.experimental import pallas as pl
from jax.experimental.pallas import tpu as pltpu
from jax.sharding import PartitionSpec as P

NKG = 64
NC_LANES = 128
MESH = pl.DeviceIdType.MESH
F32, BF16 = jnp.float32, jnp.bfloat16


def iota(shape, axis):
    return lax.broadcasted_iota(jnp.int32, shape, axis)


def each(n, f):
    if n <= 8:
        for i in range(1, n):
            f(i)
    else:
        pl.loop(1, n)(f)


def kernel(
    dims, pol, blk, coords, kidx, gap, coup, weight, out,
    stage, gath, coups, part, rate,
    w_send, w_recv, c_send, c_recv, p_send, p_recv, r_send, r_recv,
):
    ren, kan = dims
    re, ka = lax.axis_index("re"), lax.axis_index("ka")
    own_r = blk.shape[0]
    cols = blk.shape[3]
    half = stage.shape[0]
    group = NC_LANES // half
    count = kidx.shape[1]
    nb = gap.shape[1]
    nv = cols // nb
    modes, nc = coup.shape[1], coup.shape[3]
    mh = modes // 2
    rows = mh * nc
    q_own = coup.shape[0]
    qn = kan * q_own
    kv = nv * count

    barrier = pltpu.get_barrier_semaphore()

    def peer(n, me, i):
        return lax.rem(me + i, n)

    def hello_ka(i):
        pl.semaphore_signal(barrier, inc=1, device_id={"ka": peer(kan, ka, i)}, device_id_type=MESH)

    def hello_re(i):
        pl.semaphore_signal(barrier, inc=1, device_id={"re": peer(ren, re, i)}, device_id_type=MESH)

    each(kan, hello_ka)
    each(ren, hello_re)

    stage[...] = jnp.zeros_like(stage)
    for r in range(own_r):
        stage[2 * r : 2 * r + 2, :] = (
            blk[r, 0].astype(F32) * pol[0] + blk[r, 1].astype(F32) * pol[1] + blk[r, 2].astype(F32) * pol[2]
        )
    base = lax.rem(ka, group) * half
    spot = iota((own_r, NC_LANES), 1) - base - 2 * iota((own_r, NC_LANES), 0)
    spread = jnp.where((spot == 0) | (spot == 1), 1.0, 0.0).astype(BF16)
    stage[2 * own_r : 2 * own_r + 3, 0:NC_LANES] = jnp.dot(
        coords[...].astype(F32).astype(BF16), spread, preferred_element_type=F32
    )
    whole = stage[...]
    high = whole.astype(BF16)
    gath[ka, 0:half, :] = high
    gath[ka, half:, :] = (whole - high.astype(F32)).astype(BF16)

    for q in range(q_own):
        pieces = [
            coup[q, h * mh : (h + 1) * mh, part_of].astype(F32).reshape(rows, nb)
            for h in range(2)
            for part_of in range(2)
        ]
        coups[ka * q_own + q, 0:rows, :] = jnp.concatenate(pieces, axis=1).astype(BF16)
        wide = jnp.broadcast_to(weight[q : q + 1, :].astype(F32), (16, modes))
        line, lane = iota((16, modes), 0), iota((16, modes), 1)
        w0 = jnp.sum(jnp.where((lane == line) & (line < mh), wide, 0.0), axis=1, keepdims=True)
        w1 = jnp.sum(jnp.where((lane == line + mh) & (line < mh), wide, 0.0), axis=1, keepdims=True)
        coups[ka * q_own + q, rows:, :] = jnp.where(
            iota((16, NC_LANES), 1) < NC_LANES // 2, w0, w1
        ).astype(BF16)

    pl.semaphore_wait(barrier, kan - 1 + ren - 1)

    def w_copy(i):
        return pltpu.make_async_remote_copy(
            gath.at[ka], gath.at[ka], w_send.at[i], w_recv.at[ka],
            device_id={"ka": peer(kan, ka, i)}, device_id_type=MESH,
        )

    def c_copy(i):
        mine = coups.at[pl.ds(ka * q_own, q_own)]
        return pltpu.make_async_remote_copy(
            mine, mine, c_send.at[i], c_recv.at[ka],
            device_id={"ka": peer(kan, ka, i)}, device_id_type=MESH,
        )

    each(kan, lambda i: w_copy(i).start())
    each(kan, lambda i: c_copy(i).start())

    square = iota((count, count), 0) == iota((count, count), 1)
    kcols = [
        jnp.sum(jnp.where(square, jnp.broadcast_to(kidx[d : d + 1, :].astype(F32), (count, count)), 0.0),
                axis=1, keepdims=True)
        for d in range(3)
    ]

    def w_wait(i):
        slot = peer(kan, ka, i)
        pltpu.make_async_remote_copy(
            gath.at[slot], gath.at[slot], w_send.at[i], w_recv.at[slot],
            device_id={"ka": slot}, device_id_type=MESH,
        ).wait_recv()

    each(kan, w_wait)

    lanes = iota((count, group * half), 1)
    inside = lax.rem(lanes, half)
    used = inside < 2 * own_r
    even = lax.rem(lanes, 2) == 0

    def partial_of(g):
        block = gath[pl.ds(g * group, group)]
        where = block[:, 0:half, 0:NC_LANES].astype(F32)
        here = jnp.sum(where, axis=0)[2 * own_r : 2 * own_r + 3]
        turns = kcols[0] * here[0:1] + kcols[1] * here[1:2] + kcols[2] * here[2:3]
        turns = turns - NKG * jnp.floor(turns * (1.0 / NKG))
        angle = turns * (2.0 * math.pi / NKG)
        cosine = jnp.where(used, jnp.cos(angle), 0.0)
        sine = jnp.where(used, jnp.sin(angle), 0.0)
        left = jnp.concatenate(
            [jnp.where(even, cosine, -sine), jnp.where(even, sine, cosine)], axis=0
        ).astype(BF16)
        return jnp.dot(
            left, block[:, 0:half].reshape(group * half, cols), preferred_element_type=F32
        ) + jnp.dot(left, block[:, half:].reshape(group * half, cols), preferred_element_type=F32)

    if kan == group:
        part[re] = partial_of(0)
    else:
        part[re] = partial_of(0)

        @pl.loop(1, kan // group)
        def _(g):
            part[re] += partial_of(g)

    def p_copy(i):
        return pltpu.make_async_remote_copy(
            part.at[re], part.at[re], p_send.at[i], p_recv.at[re],
            device_id={"re": peer(ren, re, i)}, device_id_type=MESH,
        )

    each(ren, lambda i: p_copy(i).start())

    gaps = jnp.concatenate([gap[...]] * nv, axis=1)
    kv2 = 2 * kv
    pick = jnp.where(
        lax.rem(iota((kv2, NC_LANES), 0), count) == iota((kv2, NC_LANES), 1), 1.0, 0.0
    ).astype(BF16)

    def p_wait(i):
        slot = peer(ren, re, i)
        pltpu.make_async_remote_copy(
            part.at[slot], part.at[slot], p_send.at[i], p_recv.at[slot],
            device_id={"re": slot}, device_id_type=MESH,
        ).wait_recv()

    each(ren, p_wait)
    total = part[0]
    for i in range(1, ren):
        total = total + part[i]
    real = total[0:count] / gaps
    imag = total[count:] / gaps
    per = NC_LANES // nb
    lane = iota((count, NC_LANES), 1)

    def rolled(x):
        tiles = [x[:, t * NC_LANES : (t + 1) * NC_LANES] for t in range(cols // NC_LANES)]
        return [[pltpu.roll(t, nb * s, 1) if s else t for s in range(per)] for t in tiles]

    reals, imags = rolled(real), rolled(imag)

    def rows_of(first, second, sign, h):
        blocks = []
        for v in range(nv):
            a = first[v // per][(2 * h - v) % per]
            b = second[v // per][(2 * h + 1 - v) % per]
            start = 2 * h * nb
            x = jnp.where(lane < start + nb, a, sign * b)
            blocks.append(jnp.where((lane >= start) & (lane < start + 2 * nb), x, 0.0))
        return blocks

    left = jnp.concatenate(
        rows_of(reals, imags, -1.0, 0) + rows_of(reals, imags, -1.0, 1)
        + rows_of(imags, reals, 1.0, 0) + rows_of(imags, reals, 1.0, 1),
        axis=0,
    ).astype(BF16)

    def c_wait(i):
        slot = peer(kan, ka, i)
        there = coups.at[pl.ds(slot * q_own, q_own)]
        pltpu.make_async_remote_copy(
            there, there, c_send.at[i], c_recv.at[slot],
            device_id={"ka": slot}, device_id_type=MESH,
        ).wait_recv()

    each(kan, c_wait)
    many = math.gcd(qn, 8)

    def rates_of(g):
        held = coups[pl.ds(g * many, many)]
        amp = lax.dot_general(
            held[:, 0:rows].reshape(many * rows, NC_LANES), left,
            (((1,), (1,)), ((), ())), preferred_element_type=F32,
        )
        lines = []
        for q in range(many):
            w = held[q, rows:].astype(F32)
            w_lanes = jnp.concatenate(
                [jnp.broadcast_to(w[:, 0:1], (16, kv)), jnp.broadcast_to(w[:, NC_LANES - 1 :], (16, kv))], axis=1
            )
            acc = None
            for i in range(mh):
                at = q * rows + i * nc
                a, b = amp[at : at + nc, 0:kv2], amp[at : at + nc, kv2:]
                term = (a * a + b * b) * w_lanes[i : i + 1]
                acc = term if acc is None else acc + term
            lines.append(jnp.sum(acc, axis=0, keepdims=True))
        flat = jnp.concatenate(lines, axis=0)
        got = None
        for _ in range(3):
            head = flat.astype(BF16)
            flat = flat - head.astype(F32)
            piece = jnp.dot(head, pick, preferred_element_type=F32)
            got = piece if got is None else got + piece
        rate[re, pl.ds(pl.multiple_of(g * many, many), many), :] = got

    if qn == many:
        rates_of(0)
    else:
        pl.loop(0, qn // many)(rates_of)

    def r_copy(i):
        return pltpu.make_async_remote_copy(
            rate.at[re], rate.at[re], r_send.at[i], r_recv.at[re],
            device_id={"re": peer(ren, re, i)}, device_id_type=MESH,
        )

    each(ren, lambda i: r_copy(i).start())

    def r_wait(i):
        slot = peer(ren, re, i)
        pltpu.make_async_remote_copy(
            rate.at[slot], rate.at[slot], r_send.at[i], r_recv.at[slot],
            device_id={"re": slot}, device_id_type=MESH,
        ).wait_recv()

    each(kan, lambda i: w_copy(i).wait_send())
    each(kan, lambda i: c_copy(i).wait_send())
    each(ren, lambda i: p_copy(i).wait_send())
    each(ren, r_wait)
    q_out = out.shape[0]
    mine = pl.ds(re * q_out, q_out)
    summed = rate[0, mine, :]
    for i in range(1, ren):
        summed = summed + rate[i, mine, :]
    out[...] = summed[:, 0:count] * (1.0 / (modes * ren * nv * nc))
    each(ren, lambda i: r_copy(i).wait_send())


def body(dims, lattice_blocks, lattice_coords, kpoint_index, polarization, energy_gap, coupling, phonon_weight):
    ren, kan = dims
    own_r, _, _, cols = lattice_blocks.shape
    count = kpoint_index.shape[0]
    q_own, modes, _, _, nc = coupling.shape
    rows = modes // 2 * nc
    half = 16 * pl.cdiv(2 * own_r + 3, 16)
    qn = q_own * kan
    vmem = pl.BlockSpec(memory_space=pltpu.VMEM)
    dma = pltpu.SemaphoreType.DMA
    rates = pl.pallas_call(
        functools.partial(kernel, dims),
        out_shape=jax.ShapeDtypeStruct((qn // ren, count), F32),
        in_specs=[pl.BlockSpec(memory_space=pltpu.SMEM)] + [vmem] * 6,
        out_specs=vmem,
        scratch_shapes=[
            pltpu.VMEM((half, cols), F32),
            pltpu.VMEM((kan, 2 * half, cols), BF16),
            pltpu.VMEM((qn, rows + 16, NC_LANES), BF16),
            pltpu.VMEM((ren, 2 * count, cols), F32),
            pltpu.VMEM((ren, qn, NC_LANES), F32),
            dma((kan,)), dma((kan,)), dma((kan,)), dma((kan,)),
            dma((ren,)), dma((ren,)), dma((ren,)), dma((ren,)),
        ],
        compiler_params=pltpu.CompilerParams(collective_id=0, has_side_effects=True),
    )(
        polarization,
        lattice_blocks.transpose(0, 2, 1, 3),
        lattice_coords.T,
        kpoint_index.T,
        energy_gap,
        coupling.transpose(0, 1, 2, 4, 3),
        phonon_weight,
    )
    return rates.T


def solution(mesh):
    dims = (mesh.shape["re"], mesh.shape["ka"])
    return jax.shard_map(
        functools.partial(body, dims),
        mesh=mesh,
        in_specs=(
            P(("re", "ka"), None, None, None),
            P(("re", "ka"), None),
            P("ka", None),
            P(),
            P("ka", None),
            P("ka", "re", None, None, None),
            P("ka", "re"),
        ),
        out_specs=P("ka", "re"),
        check_vma=False,
    )
```

```python
import functools
import math

import jax
import jax.numpy as jnp
from jax import lax
from jax.experimental import pallas as pl
from jax.experimental.pallas import tpu as pltpu
from jax.sharding import PartitionSpec as P

NKG = 64
NC_LANES = 128
MESH = pl.DeviceIdType.MESH
F32, BF16 = jnp.float32, jnp.bfloat16


def iota(shape, axis):
    return lax.broadcasted_iota(jnp.int32, shape, axis)


def each(n, f):
    if n <= 8:
        for i in range(1, n):
            f(i)
    else:
        pl.loop(1, n)(f)


def kernel(
    dims, pol, blk, coords, kidx, gap, coup, weight, out,
    stage, gath, gpart, gall, part,
    w_send, w_recv, g_send, g_recv, b_send, b_recv, p_send, p_recv,
):
    ren, kan = dims
    re, ka = lax.axis_index("re"), lax.axis_index("ka")
    own_r = blk.shape[0]
    cols = blk.shape[3]
    half = stage.shape[0]
    group = NC_LANES // half
    count = kidx.shape[1]
    nb = gap.shape[1]
    nv = cols // nb
    modes, nc = coup.shape[1], coup.shape[3]
    rows = modes * nc
    q_own = coup.shape[0]
    q_out = out.shape[0]
    tall = nb // 2
    owner = (ka * q_own) // q_out
    spot_out = lax.rem(ka * q_own, q_out)

    barrier = pltpu.get_barrier_semaphore()

    def peer(n, me, i):
        return lax.rem(me + i, n)

    def hello_ka(i):
        pl.semaphore_signal(barrier, inc=1, device_id={"ka": peer(kan, ka, i)}, device_id_type=MESH)

    def hello_re(i):
        pl.semaphore_signal(barrier, inc=1, device_id={"re": peer(ren, re, i)}, device_id_type=MESH)

    each(kan, hello_ka)
    each(ren, hello_re)

    stage[...] = jnp.zeros_like(stage)
    for r in range(own_r):
        stage[2 * r : 2 * r + 2, :] = (
            blk[r, 0].astype(F32) * pol[0] + blk[r, 1].astype(F32) * pol[1] + blk[r, 2].astype(F32) * pol[2]
        )
    base = lax.rem(ka, group) * half
    spot = iota((own_r, NC_LANES), 1) - base - 2 * iota((own_r, NC_LANES), 0)
    spread = jnp.where((spot == 0) | (spot == 1), 1.0, 0.0).astype(BF16)
    stage[2 * own_r : 2 * own_r + 3, 0:NC_LANES] = jnp.dot(
        coords[...].astype(F32).astype(BF16), spread, preferred_element_type=F32
    )
    whole = stage[...]
    high = whole.astype(BF16)
    gath[ka, 0:half, :] = high
    gath[ka, half:, :] = (whole - high.astype(F32)).astype(BF16)

    for q in range(q_own):
        flat = jnp.concatenate(
            [coup[q, :, part_of].astype(F32).reshape(rows, nb) for part_of in range(2)], axis=1
        )
        wide = jnp.broadcast_to(weight[q : q + 1, :].astype(F32), (rows, modes))
        at_mode = iota((rows, modes), 1) == iota((rows, modes), 0) // nc
        scaled = flat * jnp.sum(jnp.where(at_mode, wide, 0.0), axis=1, keepdims=True)
        top = scaled.astype(BF16)
        low = (scaled - top.astype(F32)).astype(BF16)
        flat = flat.astype(BF16)
        gram = sum(
            lax.dot_general(x, flat, (((0,), (0,)), ((), ())), preferred_element_type=F32) for x in (top, low)
        )
        same = gram[0:nb, 0:nb] + gram[nb:, nb:]
        cross = gram[nb:, 0:nb] - gram[0:nb, nb:]
        gpart[re, q * tall : (q + 1) * tall, :] = jnp.concatenate(
            [same[0:tall], cross[0:tall], same[tall:], cross[tall:]], axis=1
        )

    pl.semaphore_wait(barrier, kan - 1 + ren - 1)

    def w_copy(i):
        return pltpu.make_async_remote_copy(
            gath.at[ka], gath.at[ka], w_send.at[i], w_recv.at[ka],
            device_id={"ka": peer(kan, ka, i)}, device_id_type=MESH,
        )

    def g_copy():
        return pltpu.make_async_remote_copy(
            gpart.at[re], gpart.at[re], g_send.at[0], g_recv.at[re],
            device_id={"re": owner}, device_id_type=MESH,
        )

    def b_copy(i):
        mine = gall.at[pl.ds(spot_out, q_own)]
        return pltpu.make_async_remote_copy(
            mine, mine, b_send.at[i], b_recv.at[spot_out // q_own],
            device_id={"ka": peer(kan, ka, i)}, device_id_type=MESH,
        )

    each(kan, lambda i: w_copy(i).start())

    @pl.when(re != owner)
    def _():
        g_copy().start()


    square = iota((count, count), 0) == iota((count, count), 1)
    kcols = [
        jnp.sum(jnp.where(square, jnp.broadcast_to(kidx[d : d + 1, :].astype(F32), (count, count)), 0.0),
                axis=1, keepdims=True)
        for d in range(3)
    ]

    @pl.when(re == owner)
    def _():
        def g_wait(i):
            slot = peer(ren, re, i)
            pltpu.make_async_remote_copy(
                gpart.at[slot], gpart.at[slot], g_send.at[0], g_recv.at[slot],
                device_id={"re": slot}, device_id_type=MESH,
            ).wait_recv()

        each(ren, g_wait)
        gram = gpart[0]
        for i in range(1, ren):
            gram = gram + gpart[i]
        for q in range(q_own):
            gall[spot_out + q] = gram[q * tall : (q + 1) * tall]
        each(kan, lambda i: b_copy(i).start())

    def w_wait(i):
        slot = peer(kan, ka, i)
        pltpu.make_async_remote_copy(
            gath.at[slot], gath.at[slot], w_send.at[i], w_recv.at[slot],
            device_id={"ka": slot}, device_id_type=MESH,
        ).wait_recv()

    each(kan, w_wait)

    lanes = iota((count, group * half), 1)
    inside = lax.rem(lanes, half)
    used = inside < 2 * own_r
    even = lax.rem(lanes, 2) == 0

    def partial_of(g):
        block = gath[pl.ds(g * group, group)]
        where = block[:, 0:half, 0:NC_LANES].astype(F32)
        here = jnp.sum(where, axis=0)[2 * own_r : 2 * own_r + 3]
        turns = kcols[0] * here[0:1] + kcols[1] * here[1:2] + kcols[2] * here[2:3]
        turns = turns - NKG * jnp.floor(turns * (1.0 / NKG))
        angle = turns * (2.0 * math.pi / NKG)
        cosine = jnp.where(used, jnp.cos(angle), 0.0)
        sine = jnp.where(used, jnp.sin(angle), 0.0)
        left = jnp.concatenate(
            [jnp.where(even, cosine, -sine), jnp.where(even, sine, cosine)], axis=0
        ).astype(BF16)
        return jnp.dot(
            left, block[:, 0:half].reshape(group * half, cols), preferred_element_type=F32
        ) + jnp.dot(left, block[:, half:].reshape(group * half, cols), preferred_element_type=F32)

    if kan == group:
        part[re] = partial_of(0)
    else:
        part[re] = partial_of(0)

        @pl.loop(1, kan // group)
        def _(g):
            part[re] += partial_of(g)

    def p_copy(i):
        return pltpu.make_async_remote_copy(
            part.at[re], part.at[re], p_send.at[i], p_recv.at[re],
            device_id={"re": peer(ren, re, i)}, device_id_type=MESH,
        )

    each(ren, lambda i: p_copy(i).start())

    gaps = jnp.concatenate([gap[...]] * nv, axis=1)
    def p_wait(i):
        slot = peer(ren, re, i)
        pltpu.make_async_remote_copy(
            part.at[slot], part.at[slot], p_send.at[i], p_recv.at[slot],
            device_id={"re": slot}, device_id_type=MESH,
        ).wait_recv()

    each(ren, p_wait)
    total = part[0]
    for i in range(1, ren):
        total = total + part[i]
    real = total[0:count] / gaps
    imag = total[count:] / gaps
    per = NC_LANES // nb
    quarter = iota((count, NC_LANES), 1) // nb

    def rolled(x):
        x = x.astype(BF16).astype(F32)
        tiles = [x[:, t * NC_LANES : (t + 1) * NC_LANES] for t in range(cols // NC_LANES)]
        return [[pltpu.roll(t, nb * s, 1) if s else t for s in range(per)] for t in tiles]

    reals, imags = rolled(real), rolled(imag)
    blocks = []
    for v in range(nv):
        x = imags[v // per][(3 - v) % per]
        x = jnp.where(quarter == 2, reals[v // per][(2 - v) % per], x)
        x = jnp.where(quarter == 1, imags[v // per][(1 - v) % per], x)
        blocks.append(jnp.where(quarter == 0, reals[v // per][(0 - v) % per], x))
    left = jnp.concatenate(blocks, axis=0)
    left16 = left.astype(BF16)

    first = (re * q_out) // q_own
    for step in range(q_out // q_own):

        @pl.when(first + step != ka)
        def _():
            there = gall.at[pl.ds(step * q_own, q_own)]
            pltpu.make_async_remote_copy(
                there, there, b_send.at[0], b_recv.at[step],
                device_id={"ka": first + step}, device_id_type=MESH,
            ).wait_recv()

    def square_of(packed):
        a, b = packed[:, 0 : 2 * nb], packed[:, 2 * nb :]
        rows_of = jnp.concatenate([a, b], axis=0)
        same, cross = rows_of[:, 0:nb], rows_of[:, nb:]
        return jnp.concatenate(
            [rows_of, jnp.concatenate([-cross, same], axis=1)], axis=0
        )

    scale = 1.0 / (modes * ren * nv * nc)
    choose = jnp.where(iota((8, NC_LANES), 1) // (2 * nb) == iota((8, NC_LANES), 0), 1.0, 0.0).astype(BF16)
    for pair in range(q_out // 2):
        right = jnp.concatenate([square_of(gall[2 * pair]), square_of(gall[2 * pair + 1])], axis=1)
        top = right.astype(BF16)
        low = (right - top.astype(F32)).astype(BF16)
        power = left * jnp.dot(
            left16, jnp.concatenate([top, low], axis=0), preferred_element_type=F32
        )
        summed = power[0:count]
        for v in range(1, nv):
            summed = summed + power[v * count : (v + 1) * count]
        got = None
        for _ in range(3):
            head = summed.astype(BF16)
            summed = summed - head.astype(F32)
            piece = lax.dot_general(choose, head, (((1,), (1,)), ((), ())), preferred_element_type=F32)
            got = piece if got is None else got + piece
        out[2 * pair : 2 * pair + 2, :] = got[0:2] * scale

    each(kan, lambda i: w_copy(i).wait_send())
    each(ren, lambda i: p_copy(i).wait_send())

    @pl.when(re != owner)
    def _():
        g_copy().wait_send()

    @pl.when(re == owner)
    def _():
        each(kan, lambda i: b_copy(i).wait_send())


def body(dims, lattice_blocks, lattice_coords, kpoint_index, polarization, energy_gap, coupling, phonon_weight):
    ren, kan = dims
    own_r, _, _, cols = lattice_blocks.shape
    count = kpoint_index.shape[0]
    q_own = coupling.shape[0]
    tall = energy_gap.shape[1] // 2
    half = 16 * pl.cdiv(2 * own_r + 3, 16)
    q_out = q_own * kan // ren
    vmem = pl.BlockSpec(memory_space=pltpu.VMEM)
    dma = pltpu.SemaphoreType.DMA
    rates = pl.pallas_call(
        functools.partial(kernel, dims),
        out_shape=jax.ShapeDtypeStruct((q_out, count), F32),
        in_specs=[pl.BlockSpec(memory_space=pltpu.SMEM)] + [vmem] * 6,
        out_specs=vmem,
        scratch_shapes=[
            pltpu.VMEM((half, cols), F32),
            pltpu.VMEM((kan, 2 * half, cols), BF16),
            pltpu.VMEM((ren, q_own * tall, NC_LANES), F32),
            pltpu.VMEM((q_out, tall, NC_LANES), F32),
            pltpu.VMEM((ren, 2 * count, cols), F32),
            dma((kan,)), dma((kan,)), dma((1,)), dma((ren,)),
            dma((kan,)), dma((q_out // q_own,)), dma((ren,)), dma((ren,)),
        ],
        compiler_params=pltpu.CompilerParams(collective_id=0, has_side_effects=True),
    )(
        polarization,
        lattice_blocks.transpose(0, 2, 1, 3),
        lattice_coords.T,
        kpoint_index.T,
        energy_gap,
        coupling.transpose(0, 1, 2, 4, 3),
        phonon_weight,
    )
    return rates.T


def solution(mesh):
    dims = (mesh.shape["re"], mesh.shape["ka"])
    return jax.shard_map(
        functools.partial(body, dims),
        mesh=mesh,
        in_specs=(
            P(("re", "ka"), None, None, None),
            P(("re", "ka"), None),
            P("ka", None),
            P(),
            P("ka", None),
            P("ka", "re", None, None, None),
            P("ka", "re"),
        ),
        out_specs=P("ka", "re"),
        check_vma=False,
    )
```

```python
import functools
import math

import jax
import jax.numpy as jnp
from jax import lax
from jax.experimental import pallas as pl
from jax.experimental.pallas import tpu as pltpu
from jax.sharding import PartitionSpec as P

NKG = 64
NC_LANES = 128
MESH = pl.DeviceIdType.MESH
F32, BF16 = jnp.float32, jnp.bfloat16


def iota(shape, axis):
    return lax.broadcasted_iota(jnp.int32, shape, axis)


def each(n, f):
    if n <= 8:
        for i in range(1, n):
            f(i)
    else:
        pl.loop(1, n)(f)


def circle(turns):
    turns = turns - NKG * jnp.floor(turns * (1.0 / NKG) + 0.5)
    size = jnp.abs(turns)

    def sine_of(x):
        x = x * (2.0 * math.pi / NKG)
        y = x * x
        z = 1.0 / 6227020800.0
        for c in (-1.0 / 39916800.0, 1.0 / 362880.0, -1.0 / 5040.0, 1.0 / 120.0, -1.0 / 6.0, 1.0):
            z = z * y + c
        return x * z

    sine = sine_of(jnp.minimum(size, NKG // 2 - size))
    return sine_of(NKG // 4 - size), jnp.where(turns < 0, -sine, sine)


def kernel(
    dims, pol_in, blk_in, coords_in, kidx_in, gap_in, coup_in, weight_in, out,
    pol, blk, coords, kidx, gap, coup, weight, in_sem, stage, gath, gpart, gall, part,
    w_send, w_recv, g_send, g_recv, b_send, b_recv, p_send, p_recv,
):
    ren, kan = dims
    re, ka = lax.axis_index("re"), lax.axis_index("ka")
    own_r = blk.shape[0]
    cols = blk.shape[3]
    half = stage.shape[0]
    group = NC_LANES // half
    count = kidx.shape[1]
    nb = gap.shape[1]
    nv = cols // nb
    modes, nc = coup.shape[1], coup.shape[3]
    rows = modes * nc
    q_own = coup.shape[0]
    q_out = out.shape[0]
    tall = nb // 2
    owner = (ka * q_own) // q_out
    spot_out = lax.rem(ka * q_own, q_out)

    barrier = pltpu.get_barrier_semaphore()

    def peer(n, me, i):
        return lax.rem(me + i, n)

    def hello_ka(i):
        pl.semaphore_signal(barrier, inc=1, device_id={"ka": peer(kan, ka, i)}, device_id_type=MESH)

    def hello_re(i):
        pl.semaphore_signal(barrier, inc=1, device_id={"re": peer(ren, re, i)}, device_id_type=MESH)

    each(kan, hello_ka)
    each(ren, hello_re)

    loads = [
        pltpu.make_async_copy(source, to, in_sem.at[i])
        for i, (source, to) in enumerate([
            (blk_in, blk), (coords_in, coords), (pol_in, pol), (coup_in, coup),
            (weight_in, weight), (kidx_in, kidx), (gap_in, gap),
        ])
    ]
    for load in loads:
        load.start()

    stage[...] = jnp.zeros_like(stage)
    for load in loads[:3]:
        load.wait()
    for r in range(own_r):
        stage[2 * r : 2 * r + 2, :] = (
            blk[r, 0].astype(F32) * pol[0] + blk[r, 1].astype(F32) * pol[1] + blk[r, 2].astype(F32) * pol[2]
        )
    base = lax.rem(ka, group) * half
    spot = iota((own_r, NC_LANES), 1) - base - 2 * iota((own_r, NC_LANES), 0)
    spread = jnp.where((spot == 0) | (spot == 1), 1.0, 0.0).astype(BF16)
    stage[2 * own_r : 2 * own_r + 3, 0:NC_LANES] = jnp.dot(
        coords[...].astype(F32).astype(BF16), spread, preferred_element_type=F32
    )
    whole = stage[...]
    high = whole.astype(BF16)
    gath[ka, 0:half, :] = high

    for load in loads[3:]:
        load.wait()
    for q in range(q_own):
        flat = jnp.concatenate(
            [coup[q, :, part_of].astype(F32).reshape(rows, nb) for part_of in range(2)], axis=1
        )
        wide = jnp.broadcast_to(weight[q : q + 1, :].astype(F32), (rows, modes))
        at_mode = iota((rows, modes), 1) == iota((rows, modes), 0) // nc
        scaled = flat * jnp.sum(jnp.where(at_mode, wide, 0.0), axis=1, keepdims=True)
        top = scaled.astype(BF16)
        low = (scaled - top.astype(F32)).astype(BF16)
        flat = flat.astype(BF16)
        gram = sum(
            lax.dot_general(x, flat, (((0,), (0,)), ((), ())), preferred_element_type=F32) for x in (top, low)
        )
        same = gram[0:nb, 0:nb] + gram[nb:, nb:]
        cross = gram[nb:, 0:nb] - gram[0:nb, nb:]
        gpart[re, q * tall : (q + 1) * tall, :] = jnp.concatenate(
            [same[0:tall], cross[0:tall], same[tall:], cross[tall:]], axis=1
        )

    pl.semaphore_wait(barrier, kan - 1 + ren - 1)

    def w_copy(i):
        return pltpu.make_async_remote_copy(
            gath.at[ka], gath.at[ka], w_send.at[i], w_recv.at[ka],
            device_id={"ka": peer(kan, ka, i)}, device_id_type=MESH,
        )

    def g_copy():
        return pltpu.make_async_remote_copy(
            gpart.at[re], gpart.at[re], g_send.at[0], g_recv.at[re],
            device_id={"re": owner}, device_id_type=MESH,
        )

    def b_copy(i):
        mine = gall.at[pl.ds(spot_out, q_own)]
        return pltpu.make_async_remote_copy(
            mine, mine, b_send.at[i], b_recv.at[spot_out // q_own],
            device_id={"ka": peer(kan, ka, i)}, device_id_type=MESH,
        )

    each(kan, lambda i: w_copy(i).start())

    @pl.when(re != owner)
    def _():
        g_copy().start()


    square = iota((count, count), 0) == iota((count, count), 1)
    kcols = [
        jnp.sum(jnp.where(square, jnp.broadcast_to(kidx[d : d + 1, :].astype(F32), (count, count)), 0.0),
                axis=1, keepdims=True)
        for d in range(3)
    ]

    @pl.when(re == owner)
    def _():
        def g_wait(i):
            slot = peer(ren, re, i)
            pltpu.make_async_remote_copy(
                gpart.at[slot], gpart.at[slot], g_send.at[0], g_recv.at[slot],
                device_id={"re": slot}, device_id_type=MESH,
            ).wait_recv()

        each(ren, g_wait)
        gram = gpart[0]
        for i in range(1, ren):
            gram = gram + gpart[i]
        for q in range(q_own):
            gall[spot_out + q] = gram[q * tall : (q + 1) * tall]
        each(kan, lambda i: b_copy(i).start())

    def w_wait(i):
        slot = peer(kan, ka, i)
        pltpu.make_async_remote_copy(
            gath.at[slot], gath.at[slot], w_send.at[i], w_recv.at[slot],
            device_id={"ka": slot}, device_id_type=MESH,
        ).wait_recv()

    each(kan, w_wait)

    lanes = iota((count, group * half), 1)
    inside = lax.rem(lanes, half)
    used = inside < 2 * own_r
    even = lax.rem(lanes, 2) == 0

    def partial_of(g):
        block = gath[pl.ds(g * group, group)]
        where = block[:, 0:half, 0:NC_LANES].astype(F32)
        here = jnp.sum(where, axis=0)[2 * own_r : 2 * own_r + 3]
        turns = kcols[0] * here[0:1] + kcols[1] * here[1:2] + kcols[2] * here[2:3]
        cosine, sine = circle(turns)
        cosine = jnp.where(used, cosine, 0.0)
        sine = jnp.where(used, sine, 0.0)
        left = jnp.concatenate(
            [jnp.where(even, cosine, -sine), jnp.where(even, sine, cosine)], axis=0
        ).astype(BF16)
        return jnp.dot(
            left, block[:, 0:half].reshape(group * half, cols), preferred_element_type=F32
        )

    if kan == group:
        part[re] = partial_of(0).astype(BF16)
    else:
        part[re] = partial_of(0).astype(BF16)

        @pl.loop(1, kan // group)
        def _(g):
            part[re] = (part[re].astype(F32) + partial_of(g)).astype(BF16)

    def p_copy(i):
        return pltpu.make_async_remote_copy(
            part.at[re], part.at[re], p_send.at[i], p_recv.at[re],
            device_id={"re": peer(ren, re, i)}, device_id_type=MESH,
        )

    each(ren, lambda i: p_copy(i).start())

    gaps = jnp.concatenate([gap[...]] * nv, axis=1)
    def p_wait(i):
        slot = peer(ren, re, i)
        pltpu.make_async_remote_copy(
            part.at[slot], part.at[slot], p_send.at[i], p_recv.at[slot],
            device_id={"re": slot}, device_id_type=MESH,
        ).wait_recv()

    each(ren, p_wait)
    total = part[0].astype(F32)
    for i in range(1, ren):
        total = total + part[i].astype(F32)
    real = total[0:count] / gaps
    imag = total[count:] / gaps
    per = NC_LANES // nb
    quarter = iota((count, NC_LANES), 1) // nb

    def rolled(x):
        x = x.astype(BF16).astype(F32)
        tiles = [x[:, t * NC_LANES : (t + 1) * NC_LANES] for t in range(cols // NC_LANES)]
        return [[pltpu.roll(t, nb * s, 1) if s else t for s in range(per)] for t in tiles]

    reals, imags = rolled(real), rolled(imag)
    blocks = []
    for v in range(nv):
        x = imags[v // per][(3 - v) % per]
        x = jnp.where(quarter == 2, reals[v // per][(2 - v) % per], x)
        x = jnp.where(quarter == 1, imags[v // per][(1 - v) % per], x)
        blocks.append(jnp.where(quarter == 0, reals[v // per][(0 - v) % per], x))
    left = jnp.concatenate(blocks, axis=0)
    left16 = left.astype(BF16)

    first = (re * q_out) // q_own
    for step in range(q_out // q_own):

        @pl.when(first + step != ka)
        def _():
            there = gall.at[pl.ds(step * q_own, q_own)]
            pltpu.make_async_remote_copy(
                there, there, b_send.at[0], b_recv.at[step],
                device_id={"ka": first + step}, device_id_type=MESH,
            ).wait_recv()

    def square_of(packed):
        a, b = packed[:, 0 : 2 * nb], packed[:, 2 * nb :]
        rows_of = jnp.concatenate([a, b], axis=0)
        same, cross = rows_of[:, 0:nb], rows_of[:, nb:]
        return jnp.concatenate(
            [rows_of, jnp.concatenate([-cross, same], axis=1)], axis=0
        )

    scale = 1.0 / (modes * ren * nv * nc)
    choose = jnp.where(iota((8, NC_LANES), 1) // (2 * nb) == iota((8, NC_LANES), 0), 1.0, 0.0).astype(BF16)
    for pair in range(q_out // 2):
        right = jnp.concatenate([square_of(gall[2 * pair]), square_of(gall[2 * pair + 1])], axis=1)
        top = right.astype(BF16)
        low = (right - top.astype(F32)).astype(BF16)
        power = left * jnp.dot(
            left16, jnp.concatenate([top, low], axis=0), preferred_element_type=F32
        )
        summed = power[0:count]
        for v in range(1, nv):
            summed = summed + power[v * count : (v + 1) * count]
        got = None
        for _ in range(3):
            head = summed.astype(BF16)
            summed = summed - head.astype(F32)
            piece = lax.dot_general(choose, head, (((1,), (1,)), ((), ())), preferred_element_type=F32)
            got = piece if got is None else got + piece
        out[2 * pair : 2 * pair + 2, :] = got[0:2] * scale

    each(kan, lambda i: w_copy(i).wait_send())
    each(ren, lambda i: p_copy(i).wait_send())

    @pl.when(re != owner)
    def _():
        g_copy().wait_send()

    @pl.when(re == owner)
    def _():
        each(kan, lambda i: b_copy(i).wait_send())


def body(dims, lattice_blocks, lattice_coords, kpoint_index, polarization, energy_gap, coupling, phonon_weight):
    ren, kan = dims
    own_r, _, _, cols = lattice_blocks.shape
    count = kpoint_index.shape[0]
    q_own = coupling.shape[0]
    tall = energy_gap.shape[1] // 2
    half = 16 * pl.cdiv(2 * own_r + 3, 16)
    q_out = q_own * kan // ren
    vmem = pl.BlockSpec(memory_space=pltpu.VMEM)
    dma = pltpu.SemaphoreType.DMA
    args = (
        polarization,
        lattice_blocks.transpose(0, 2, 1, 3),
        lattice_coords.T,
        kpoint_index.T,
        energy_gap,
        coupling.transpose(0, 1, 2, 4, 3),
        phonon_weight,
    )
    rates = pl.pallas_call(
        functools.partial(kernel, dims),
        out_shape=pltpu.VMEM((q_out, count), F32),
        in_specs=[pl.BlockSpec(memory_space=pl.ANY)] * len(args),
        out_specs=vmem,
        scratch_shapes=[pltpu.SMEM(polarization.shape, F32)]
        + [pltpu.VMEM(x.shape, x.dtype) for x in args[1:]]
        + [
            dma((len(args),)),
            pltpu.VMEM((half, cols), F32),
            pltpu.VMEM((kan, half, cols), BF16),
            pltpu.VMEM((ren, q_own * tall, NC_LANES), F32),
            pltpu.VMEM((q_out, tall, NC_LANES), F32),
            pltpu.VMEM((ren, 2 * count, cols), BF16),
            dma((kan,)), dma((kan,)), dma((1,)), dma((ren,)),
            dma((kan,)), dma((q_out // q_own,)), dma((ren,)), dma((ren,)),
        ],
        compiler_params=pltpu.CompilerParams(collective_id=0, has_side_effects=True),
    )(*args)
    return rates.T


def solution(mesh):
    dims = (mesh.shape["re"], mesh.shape["ka"])
    return jax.shard_map(
        functools.partial(body, dims),
        mesh=mesh,
        in_specs=(
            P(("re", "ka"), None, None, None),
            P(("re", "ka"), None),
            P("ka", None),
            P(),
            P("ka", None),
            P("ka", "re", None, None, None),
            P("ka", "re"),
        ),
        out_specs=P("ka", "re"),
        check_vma=False,
    )
```
